128 devices in a mesh: band: 64 (over y, z_lo, x, core), ga: 2 (over z_hi).
Axes of the slice: x: 4, y: 4, z: 4 (z_hi: 2, z_lo: 2; z = z_hi * 2 + z_lo), core: 2. Of those that a mesh axis runs over, the one named last changes fastest.
Arguments:
- matrix_elements: float32 [2, 16384, 12288], P(None, 'band', 'ga'), may hold values from -16 to 16
- band_index: int32 [16384], P('band'), may hold values from 0 to 1048575
- occupied: int32 [1], replicated, may hold values from 262144 to 786432
- band_weight: float32 [16384], P('band'), may hold values from 0.3 to 3
- coulomb: float32 [12288], replicated, may hold values from 0.2 to 5
Outputs:
- sigma: float32 [12288, 2, 512], P(('ga', 'band'))
The draws below stay inside these ranges and needn't reach their ends.
All inputs are finite; a program needn't handle non-finite values.
Results may differ from the reference program's by a relative error of at most 0.00018.
Values sent between devices are 32-bit elements; how exact they have to be, the bound alone decides.
No kernel may reach another device: no remote copies, remote signals or barrier semaphores. Data moves between devices by JAX's collectives and lax.ppermute only.
A program may use at most 192 MiB of HBM per device.

```python
import math
import jax
import jax.numpy as jnp
from jax import lax

NG = 12288
COLS = 512
NB = 16384


def place_ends(drawn, rng, least, top_value):
    index_at = [jax.random.randint(jax.random.fold_in(rng, axis), (), 0, length) for axis, length in enumerate(drawn.shape)]
    widest = drawn.shape.index(max(drawn.shape))
    neighbour = index_at[:widest] + [(index_at[widest] + 1) % drawn.shape[widest]] + index_at[widest + 1:]
    return drawn.at[tuple(index_at)].set(least).at[tuple(neighbour)].set(top_value)


def strengthened(result, own_key, source, target, blocks, factor):
    owner, partner = [(jnp.arange(result.shape[axis_at]) // (result.shape[axis_at] // blocks)).reshape([-1 if axis == axis_at else 1 for axis in range(result.ndim)]) for axis_at in (source, target)]
    chosen = jax.random.permutation(own_key, blocks)[partner]
    strong = (owner == chosen) | (owner == (partner + blocks // 2) % blocks)
    return jnp.where(strong, factor * result, result)


def shard_levels(stream_key, shape, shards, smallest, top_value):
    level, own = 1.0, jax.random.fold_in(stream_key, 6)
    for axis_at, parts in shards:
        draws = jnp.exp(jax.random.uniform(jax.random.fold_in(own, axis_at), (parts,), jnp.float32, smallest / len(shards), top_value / len(shards)))
        level = level * jnp.repeat(draws, shape[axis_at] // parts).reshape([-1 if axis == axis_at else 1 for axis in range(len(shape))])
    return level


def bell_draw_with(stream_key, shape, width, bound, cuts, heavy, dtype=jnp.bfloat16):
    drawn = width * jax.random.normal(stream_key, shape, jnp.float32)
    if cuts:
        drawn = drawn * shard_levels(stream_key, shape, cuts, -0.22, 0.18)
    return jnp.clip(strengthened(drawn, jax.random.fold_in(stream_key, 3), *heavy), -bound, bound).astype(dtype)


def setup_inputs(seed: int = 0) -> dict:
    arg_keys = jax.random.split(jax.random.key(seed), 6)
    return {
        "matrix_elements": bell_draw_with(arg_keys[0], (2, NB, NG), 1.0, 16.0, ((1, 64), (2, 2)), (1, 2, 64, 4.0), jnp.float32),
        "band_index": place_ends(jax.random.randint(arg_keys[1], (NB,), 0, 1048576), jax.random.fold_in(arg_keys[1], 1), 0, 1048575).astype(jnp.int32),
        "occupied": jax.random.randint(arg_keys[2], (1,), 262144, 786433).astype(jnp.int32),
        "band_weight": jnp.clip(jnp.exp(math.log(3.0) - 2.3025851 * jax.random.uniform(arg_keys[3], (NB,), jnp.float32) ** shard_levels(arg_keys[3], (NB,), ((0, 64),), -0.2, 0.2)), 0.3, 3.0),
        "coulomb": jnp.clip(jnp.exp(jax.random.uniform(arg_keys[4], (NG,), jnp.float32, math.log(0.2), math.log(5.0))), 0.2, 5.0),
    }


def reference(matrix_elements, band_index, occupied, band_weight, coulomb):
    occ = (band_index < occupied[0]).astype(jnp.float32)
    coef = (0.5 - occ) * band_weight
    real = matrix_elements[0]
    imag = matrix_elements[1]
    left = jnp.concatenate([coef[:, None] * real, coef[:, None] * imag], 0)
    slab_re = real[:, :COLS]
    slab_im = imag[:, :COLS]
    right = jnp.concatenate([jnp.concatenate([slab_re, slab_im], 1), jnp.concatenate([slab_im, -slab_re], 1)], 0)
    factor = 1.0 / math.sqrt(NB)
    sums = lax.dot_general(left, right, (((0,), (0,)), ((), ())), precision=lax.Precision.HIGHEST, preferred_element_type=jnp.float32) * factor
    square = 2.0 - real * real - imag * imag
    defect = jnp.dot(coef, square, precision=lax.Precision.HIGHEST, preferred_element_type=jnp.float32) * factor
    weight = jnp.sqrt(coulomb[:, None] * coulomb[None, :COLS])
    part_re = weight * (sums[:, :COLS] + 0.5 * (defect[:, None] + defect[None, :COLS]))
    part_im = weight * sums[:, COLS:]
    return jnp.stack([part_re, part_im], 1)
```

```python
import functools
import math

import jax
import jax.numpy as jnp
from jax import lax
from jax.experimental import pallas as pl
from jax.experimental.pallas import tpu as pltpu
from jax.sharding import Mesh
from jax.sharding import PartitionSpec as P

COLS = 512
LANES = 128
AXES = ("y", "zl", "x", "core", "ga")
SIZES = (4, 2, 4, 2, 2)


def index_of(pos):
    out = 0
    for p, n in zip(pos, SIZES):
        out = out * n + p
    return out


def pairs_of(move):
    pairs = []
    for y in range(4):
        for zl in range(2):
            for x in range(4):
                for core in range(2):
                    for ga in range(2):
                        to = move(y, zl, x, core, ga)
                        if to is not None:
                            pairs.append((index_of((y, zl, x, core, ga)), index_of(to)))
    return pairs


def send(v, move):
    return lax.ppermute(v, AXES, pairs_of(move))


def along(stage, step):
    def move(y, zl, x, core, ga):
        if (core == 0) == (stage == 1):
            return (y, zl, (x + step) % 4, core, ga)
        return ((y + step) % 4, zl, x, core, ga)

    return move


def swap_core(y, zl, x, core, ga):
    return (y, zl, x, 1 - core, ga)


def swap_z(y, zl, x, core, ga):
    return (y, 1 - zl, x, core, ga)


def slab_own(y, zl, x, core, ga):
    return (y, zl, x, core, 1) if ga == 0 else None


def slab_cross(y, zl, x, core, ga):
    return (y, zl, x, 1 - core, 1) if ga == 0 else None


def mm_kernel(
    pos, own, par, own_slab, par_slab, own_far, par_far, coefs,
    r1, l1, k0, k1, k3, right_hi, right_lo, col_def, blocks,
):
    core, first, second, ga = pos[1], pos[2], pos[3], pos[4]
    bands = own.shape[1]
    step = pl.program_id(0)

    @pl.when(step == 0)
    def _():
        total = jnp.zeros((LANES, 1), jnp.float32)
        for which, (near, far) in enumerate(((own_slab, own_far), (par_slab, par_far))):
            coef = coefs[which]
            local = ga == 0
            re = jnp.where(local, near[0], far[0])
            im = jnp.where(local, near[1], far[1])
            defect = coef * (1.0 - 0.5 * (re * re + im * im))
            total = total + jnp.sum(defect.T, axis=1, keepdims=True)
            re_t = (coef * re).T
            im_t = (coef * im).T
            side = jnp.concatenate(
                [jnp.concatenate([re_t, im_t], 1), jnp.concatenate([im_t, -re_t], 1)], 0
            )
            hi = side.astype(jnp.bfloat16)
            at = pl.ds(which * 2 * bands, 2 * bands)
            right_hi[:, at] = hi
            right_lo[:, at] = (side - hi.astype(jnp.float32)).astype(jnp.bfloat16)
        col_def[...] = jnp.broadcast_to(total, col_def.shape)

    width = own.shape[2]
    acc = None
    row_def = None
    for which, left in enumerate((own, par)):
        value = left[...].reshape(2 * bands, width)
        hi = value.astype(jnp.bfloat16)
        lo = (value - hi.astype(jnp.float32)).astype(jnp.bfloat16)
        at = pl.ds(which * 2 * bands, 2 * bands)
        dot = functools.partial(jnp.dot, preferred_element_type=jnp.float32)
        term = dot(right_hi[:, at], hi) + dot(right_hi[:, at], lo) + dot(right_lo[:, at], hi)
        acc = term if acc is None else acc + term
        parts = []
        for tile in range(width // LANES):
            lanes = pl.ds(tile * LANES, LANES)
            re, im = left[0, :, lanes], left[1, :, lanes]
            d = coefs[which] * (1.0 - 0.5 * (re * re + im * im))
            parts.append(jnp.sum(d, axis=0, keepdims=True))
        part = jnp.concatenate(parts, 1)
        row_def = part if row_def is None else row_def + part

    lane = lax.broadcasted_iota(jnp.int32, (LANES, LANES), 1)
    low = lane < LANES // 2
    tiles = []
    for tile in range(width // LANES):
        lanes = slice(tile * LANES, (tile + 1) * LANES)
        top = acc[:LANES, lanes] + (row_def[:, lanes] + col_def[...])
        tiles.append((top, acc[LANES:, lanes]))
    for pair in range(width // (3 * LANES)):
        t0, t1, t2 = tiles[3 * pair : 3 * pair + 3]
        turned = (pltpu.roll(t1[0], LANES // 2, 1), pltpu.roll(t1[1], LANES // 2, 1))
        even = (t0[0], t0[1], jnp.where(low, t1[0], turned[1]))
        odd = (t2[0], t2[1], jnp.where(low, turned[0], t1[1]))
        for side, three in enumerate((even, odd)):
            for n, v in enumerate(three):
                blocks[2 * pair + side, pl.ds(n * LANES, LANES), :] = v

    for x in range(4):
        p = jnp.where(core == 0, x, step)
        q = jnp.where(core == 0, step, x)
        rp = lax.rem(p - first + 4, 4)
        rq = lax.rem(q - second + 4, 4)
        half = rq // 2
        place = lax.rem(rq, 2)

        @pl.when(rp == 0)
        def _():
            k0[rq] = blocks[x]

        @pl.when((rp == 1) & (half == 0))
        def _():
            k1[place] = blocks[x]

        @pl.when((rp == 1) & (half == 1))
        def _():
            r1[1, place] = blocks[x]

        @pl.when((rp == 2) & (half == 0))
        def _():
            r1[0, place] = blocks[x]

        @pl.when((rp == 2) & (half == 1))
        def _():
            l1[0, place] = blocks[x]

        @pl.when((rp == 3) & (half == 0))
        def _():
            l1[1, place] = blocks[x]

        @pl.when((rp == 3) & (half == 1))
        def _():
            k3[place] = blocks[x]


def partial_sums(pos, own, par, own_far, par_far, coefs, chunk):
    bands, half = own.shape[1:]
    width = half // 8
    f32 = jnp.float32
    block = (3 * LANES, LANES)
    outs = [(2, 2), (2, 2), (4,), (2,), (2,)]
    near = pl.BlockSpec((2, bands, LANES), lambda i, pos: (0, 0, 2 * pos[1] + chunk))
    far = pl.BlockSpec((2, bands, LANES), lambda i, pos: (0, 0, 0))
    left = pl.BlockSpec((2, bands, width), lambda i, pos: (0, 0, 2 * i + pos[0]))

    def whole(n):
        return lambda i, pos: (0,) * n

    return pl.pallas_call(
        mm_kernel,
        out_shape=[jax.ShapeDtypeStruct(o + block, f32) for o in outs],
        grid_spec=pltpu.PrefetchScalarGridSpec(
            num_scalar_prefetch=1,
            grid=(4,),
            in_specs=[left, left, near, near, far, far, pl.BlockSpec((2, bands, LANES), whole(3))],
            out_specs=[pl.BlockSpec(o + block, whole(len(o) + 2)) for o in outs],
            scratch_shapes=[
                pltpu.VMEM((2 * LANES, 4 * bands), jnp.bfloat16),
                pltpu.VMEM((2 * LANES, 4 * bands), jnp.bfloat16),
                pltpu.VMEM((LANES, LANES), f32),
                pltpu.VMEM((4,) + block, f32),
            ],
        ),
        compiler_params=pltpu.CompilerParams(
            dimension_semantics=("arbitrary",), vmem_limit_bytes=48 * 2**20
        ),
        cost_estimate=pl.CostEstimate(
            flops=2 * 3 * 2 * LANES * 4 * bands * 4 * width,
            bytes_accessed=4 * (16 * bands * width + 16 * block[0] * block[1]),
            transcendentals=0,
        ),
        name="partial_sums",
    )(pos, own, par, own, par, own_far, par_far, coefs)


def reduce_plane(r1, l1, k0, k1, k3):
    r1r = send(r1, along(1, 1))
    l1r = send(l1, along(1, -1))
    r2r = send(k1 + r1r[0], along(1, 1))
    l2r = send(k3 + l1r[0], along(1, -1))
    mine = [k0[q] + l1r[1, q] + r2r[q] for q in range(2)]
    mine += [k0[2 + q] + r1r[1, q] + l2r[q] for q in range(2)]
    d1 = send(mine[1], along(2, 1))
    d3 = send(mine[3], along(2, -1))
    d2 = send(mine[2], along(2, 2))
    return mine[0] + d1 + d3 + d2


def finish_kernel(pos, here0, here1, there0, there1, row_coul, col_coul, keep, give):
    odd, core = pos[0], pos[1]
    for chunk, (here, there) in enumerate(((here0, there0), (here1, there1))):
        total = here[...] + there[...]
        body = total[: 2 * LANES].T
        fold = total[2 * LANES :].T
        rest = jnp.concatenate([fold[: LANES // 2], fold[LANES // 2 :]], 1)
        rows = jnp.where(
            odd == 1,
            jnp.concatenate([rest, body], 0),
            jnp.concatenate([body, rest], 0),
        )
        lanes = pl.ds(chunk * LANES, LANES)
        weight = jnp.sqrt(row_coul[...] * col_coul[:, lanes]) * (1.0 / math.sqrt(16384))
        n = rows.shape[0] // 2
        for part in range(2):
            v = weight * rows[:, part * LANES : (part + 1) * LANES]
            top, bottom = v[:n], v[n:]
            keep[part, :, lanes] = jnp.where(core == 0, top, bottom)
            give[part, :, lanes] = jnp.where(core == 0, bottom, top)


def body(matrix_elements, band_index, occupied, band_weight, coulomb):
    bands, half = matrix_elements.shape[1:]
    y, zl, x, core, ga = (lax.axis_index(a).astype(jnp.int32) for a in AXES)
    occ = (band_index < occupied[0]).astype(jnp.float32)
    coef = (0.5 - occ) * band_weight
    first = jnp.where(core == 0, x, y)
    second = jnp.where(core == 0, y, x)

    own = matrix_elements
    far = []
    for chunk in range(2):
        pieces = []
        for move, side in ((slab_own, core), (slab_cross, 1 - core)):
            cut = lax.dynamic_slice_in_dim(own, side * 2 * LANES + chunk * LANES, LANES, 2)
            pieces.append(send(cut, move))
        far.append(pieces)
    par_coef = send(coef, swap_core)
    par = send(own, swap_core)
    coefs = jnp.broadcast_to(jnp.stack([coef, par_coef])[:, :, None], (2, bands, LANES))

    here, there = [], []
    for chunk in range(2):
        for wave in range(2):
            rows_zl = 1 - zl if wave == 0 else zl
            pos = jnp.stack([rows_zl, core, first, second, ga])
            parts = partial_sums(pos, own, par, *far[chunk], coefs, chunk)
            done = reduce_plane(*parts)
            if wave == 0:
                there.append(send(done, swap_z))
            else:
                here.append(done)

    rows_chip = half // 32
    n = rows_chip // 2
    start = ga * half + y * (half // 4) + zl * (half // 8) + x * rows_chip
    row_coul = lax.dynamic_slice_in_dim(coulomb, start, rows_chip, 0)[:, None]
    col_coul = lax.dynamic_slice_in_dim(coulomb, core * 2 * LANES, 2 * LANES, 0)[None, :]
    vmem = pl.BlockSpec(memory_space=pltpu.VMEM)
    shape = jax.ShapeDtypeStruct((2, n, 2 * LANES), jnp.float32)
    keep, give = pl.pallas_call(
        finish_kernel,
        out_shape=[shape, shape],
        in_specs=[pl.BlockSpec(memory_space=pltpu.SMEM)] + [vmem] * 6,
        out_specs=[vmem, vmem],
        name="finish",
    )(jnp.stack([x % 2, core]), *here, *there, row_coul, col_coul)
    got = send(give, swap_core)
    left = jnp.where(core == 0, keep, got)
    right = jnp.where(core == 0, got, keep)
    return jnp.concatenate([left, right], 2).swapaxes(0, 1)


def solution(mesh):
    finer = Mesh(mesh.devices.reshape(SIZES), AXES)
    band = AXES[:4]
    in_specs = (P(None, band, "ga"), P(band), P(), P(band), P())
    out_specs = P(("ga",) + band, None, None)
    return jax.shard_map(body, mesh=finer, in_specs=in_specs, out_specs=out_specs, check_vma=False)
```

```python
import functools
import math

import jax
import jax.numpy as jnp
from jax import lax
from jax.experimental import pallas as pl
from jax.experimental.pallas import tpu as pltpu
from jax.sharding import Mesh
from jax.sharding import PartitionSpec as P

LANES = 128
AXES = ("y", "zl", "x", "core", "ga")
SIZES = (4, 2, 4, 2, 2)


def index_of(pos):
    out = 0
    for p, n in zip(pos, SIZES):
        out = out * n + p
    return out


def pairs_of(move):
    pairs = []
    for y in range(4):
        for zl in range(2):
            for x in range(4):
                for core in range(2):
                    for ga in range(2):
                        to = move(y, zl, x, core, ga)
                        if to is not None:
                            pairs.append((index_of((y, zl, x, core, ga)), index_of(to)))
    return pairs


def send(v, move):
    return lax.ppermute(v, AXES, pairs_of(move))


def along(stage, step):
    def move(y, zl, x, core, ga):
        if (core == 0) == (stage == 1):
            return (y, zl, (x + step) % 4, core, ga)
        return ((y + step) % 4, zl, x, core, ga)

    return move


def swap_core(y, zl, x, core, ga):
    return (y, zl, x, 1 - core, ga)


def swap_z(y, zl, x, core, ga):
    return (y, 1 - zl, x, core, ga)


def slab_own(y, zl, x, core, ga):
    return (y, zl, x, core, 1) if ga == 0 else None


def slab_cross(y, zl, x, core, ga):
    return (y, zl, x, 1 - core, 1) if ga == 0 else None


def mm_kernel(
    pos, own, par, coefs, *refs
):
    *slabs, r1, l1, k0, k1, k3, right, col_def, blocks, halves = refs
    chunks = len(slabs) // 4
    out_rows = 2 * chunks * LANES
    core, first, second, ga = pos[1], pos[2], pos[3], pos[4]
    bands, width = own.shape[1:]
    tile = 2 * LANES
    step = pl.program_id(0)

    @pl.when(step == 0)
    def _():
        for chunk in range(chunks):
            own_slab, par_slab, own_far, par_far = slabs[4 * chunk : 4 * chunk + 4]
            total = jnp.zeros((LANES, 1), jnp.float32)
            for which, (near, far) in enumerate(((own_slab, own_far), (par_slab, par_far))):
                coef = coefs[which]
                local = ga == 0
                re = jnp.where(local, near[0], far[0])
                im = jnp.where(local, near[1], far[1])
                defect = coef * (1.0 - 0.5 * (re * re + im * im))
                total = total + jnp.sum(defect.T, axis=1, keepdims=True)
                re_t = (coef * re).T
                im_t = (coef * im).T
                for part, pair in enumerate(((re_t, im_t), (im_t, -re_t))):
                    side = jnp.concatenate(pair, 1)
                    hi = side.astype(jnp.bfloat16)
                    at = pl.ds(which * 2 * bands, 2 * bands)
                    row = (2 * chunk + part) * LANES
                    right[pl.ds(row, LANES), at] = hi
                    right[pl.ds(out_rows + row, LANES), at] = (side - hi.astype(jnp.float32)).astype(
                        jnp.bfloat16
                    )
            col_def[chunk] = jnp.broadcast_to(total, (LANES, LANES))

    dot = functools.partial(jnp.dot, preferred_element_type=jnp.float32)
    lane = lax.broadcasted_iota(jnp.int32, (LANES, LANES), 1)
    low = lane < LANES // 2
    tiles = []
    for start in range(0, width, tile):
        lanes = pl.ds(start, tile)
        rows_def = None
        for which, left in enumerate((own, par)):
            squares = None
            for part in range(2):
                value = left[part, :, lanes]
                squares = value * value if squares is None else squares + value * value
                hi = value.astype(jnp.bfloat16)
                at = pl.ds((2 * which + part) * bands, bands)
                halves[0, at, lanes] = hi
                halves[1, at, lanes] = (value - hi.astype(jnp.float32)).astype(jnp.bfloat16)
            coef = jnp.concatenate([coefs[which]] * 2, 1)
            part_def = jnp.sum(coef * (1.0 - 0.5 * squares), axis=0, keepdims=True)
            rows_def = part_def if rows_def is None else rows_def + part_def
        both = dot(right[...], halves[0, :, lanes])
        acc = both[:out_rows] + both[out_rows:] + dot(right[:out_rows], halves[1, :, lanes])
        for n in range(2):
            cut = slice(n * LANES, (n + 1) * LANES)
            tiles.append((rows_def[:, cut], [acc[m * LANES : (m + 1) * LANES, cut] for m in range(2 * chunks)]))

    for pair in range(width // (3 * LANES)):
        for chunk in range(chunks):
            three = []
            for row_def, parts in tiles[3 * pair : 3 * pair + 3]:
                three.append((parts[2 * chunk] + (row_def + col_def[chunk]), parts[2 * chunk + 1]))
            t0, t1, t2 = three
            turned = (pltpu.roll(t1[0], LANES // 2, 1), pltpu.roll(t1[1], LANES // 2, 1))
            even = (t0[0], t0[1], jnp.where(low, t1[0], turned[1]))
            odd = (t2[0], t2[1], jnp.where(low, turned[0], t1[1]))
            for side, out in enumerate((even, odd)):
                for n, v in enumerate(out):
                    blocks[2 * pair + side, pl.ds((3 * chunk + n) * LANES, LANES), :] = v

    for x in range(4):
        p = jnp.where(core == 0, x, step)
        q = jnp.where(core == 0, step, x)
        rp = lax.rem(p - first + 4, 4)
        rq = lax.rem(q - second + 4, 4)
        half = rq // 2
        place = lax.rem(rq, 2)

        @pl.when(rp == 0)
        def _():
            k0[rq] = blocks[x]

        @pl.when((rp == 1) & (half == 0))
        def _():
            k1[place] = blocks[x]

        @pl.when((rp == 1) & (half == 1))
        def _():
            r1[1, place] = blocks[x]

        @pl.when((rp == 2) & (half == 0))
        def _():
            r1[0, place] = blocks[x]

        @pl.when((rp == 2) & (half == 1))
        def _():
            l1[0, place] = blocks[x]

        @pl.when((rp == 3) & (half == 0))
        def _():
            l1[1, place] = blocks[x]

        @pl.when((rp == 3) & (half == 1))
        def _():
            k3[place] = blocks[x]


def partial_sums(pos, own, par, coefs, far, chunks):
    bands, half = own.shape[1:]
    width = half // 8
    n = len(chunks)
    f32 = jnp.float32
    block = (3 * n * LANES, LANES)
    outs = [(2, 2), (2, 2), (4,), (2,), (2,)]
    left = pl.BlockSpec((2, bands, width), lambda i, pos: (0, 0, 2 * i + pos[0]))

    def whole(*shape):
        return pl.BlockSpec(shape, lambda i, pos: (0,) * len(shape))

    slab = whole(2, bands, LANES)
    in_specs = [left, left, slab]
    operands = [own, par, coefs]
    for chunk in chunks:
        near = pl.BlockSpec(
            (2, bands, LANES), lambda i, pos, chunk=chunk: (0, 0, 2 * pos[1] + chunk)
        )
        in_specs += [near, near, slab, slab]
        operands += [own, par, *far[chunk]]
    return pl.pallas_call(
        mm_kernel,
        out_shape=[jax.ShapeDtypeStruct(o + block, f32) for o in outs],
        grid_spec=pltpu.PrefetchScalarGridSpec(
            num_scalar_prefetch=1,
            grid=(4,),
            in_specs=in_specs,
            out_specs=[whole(*o, *block) for o in outs],
            scratch_shapes=[
                pltpu.VMEM((4 * n * LANES, 4 * bands), jnp.bfloat16),
                pltpu.VMEM((n, LANES, LANES), f32),
                pltpu.VMEM((4,) + block, f32),
                pltpu.VMEM((2, 4 * bands, width), jnp.bfloat16),
            ],
        ),
        compiler_params=pltpu.CompilerParams(
            dimension_semantics=("arbitrary",), vmem_limit_bytes=48 * 2**20
        ),
        cost_estimate=pl.CostEstimate(
            flops=2 * 3 * 2 * n * LANES * 4 * bands * 4 * width,
            bytes_accessed=4 * (16 * bands * width + 16 * block[0] * block[1]),
            transcendentals=0,
        ),
        name="partial_sums",
    )(pos, *operands)


def second_step(k1, k3, r1r, l1r):
    return k1 + r1r[0], k3 + l1r[0]


def gathered(k0, r1r, l1r, r2r, l2r):
    mine = [k0[q] + l1r[1, q] + r2r[q] for q in range(2)]
    return mine + [k0[2 + q] + r1r[1, q] + l2r[q] for q in range(2)]


def second_axis(blocks):
    d1 = send(blocks[1], along(2, 1))
    d3 = send(blocks[3], along(2, -1))
    d2 = send(blocks[2], along(2, 2))
    return blocks[0] + d1 + d3 + d2


def finish_kernel(pos, here, there, row_coul, col_coul, keep, give):
    odd, core = pos[0], pos[1]
    for chunk in range(2):
        at = pl.ds(chunk * 3 * LANES, 3 * LANES)
        total = here[at, :] + there[at, :]
        body = total[: 2 * LANES].T
        fold = total[2 * LANES :].T
        rest = jnp.concatenate([fold[: LANES // 2], fold[LANES // 2 :]], 1)
        rows = jnp.where(
            odd == 1,
            jnp.concatenate([rest, body], 0),
            jnp.concatenate([body, rest], 0),
        )
        lanes = pl.ds(chunk * LANES, LANES)
        weight = jnp.sqrt(row_coul[...] * col_coul[:, lanes]) * (1.0 / math.sqrt(16384))
        n = rows.shape[0] // 2
        for part in range(2):
            v = weight * rows[:, part * LANES : (part + 1) * LANES]
            top, bottom = v[:n], v[n:]
            keep[part, :, lanes] = jnp.where(core == 0, top, bottom)
            give[part, :, lanes] = jnp.where(core == 0, bottom, top)


def layer(matrix_elements, band_index, occupied, band_weight, coulomb):
    bands, half = matrix_elements.shape[1:]
    y, zl, x, core, ga = (lax.axis_index(a).astype(jnp.int32) for a in AXES)
    occ = (band_index < occupied[0]).astype(jnp.float32)
    coef = (0.5 - occ) * band_weight
    first = jnp.where(core == 0, x, y)
    second = jnp.where(core == 0, y, x)

    own = matrix_elements
    par = send(own, swap_core)
    far = []
    for chunk in range(2):
        pieces = []
        for move, side in ((slab_own, core), (slab_cross, 1 - core)):
            cut = lax.dynamic_slice_in_dim(own, side * 2 * LANES + chunk * LANES, LANES, 2)
            pieces.append(send(cut, move))
        far.append(pieces)
    par_coef = send(coef, swap_core)
    coefs = jnp.broadcast_to(jnp.stack([coef, par_coef])[:, :, None], (2, bands, LANES))

    waves = ((1 - zl, (0,)), (1 - zl, (1,)), (zl, (0, 1)))
    summed = []
    kept, came, turns = [], [], []
    for n, (rows_zl, chunks) in enumerate(waves):
        pos = jnp.stack([rows_zl, core, first, second, ga])
        r1, l1, *keep = partial_sums(pos, own, par, coefs, far, chunks)
        kept.append(keep)
        came.append((send(r1, along(1, 1)), send(l1, along(1, -1))))
    for n in range(len(turns), 3):
        turns.append(second_step(*kept[n][1:], *came[n]))
    for n in range(3):
        r2r = send(turns[n][0], along(1, 1))
        l2r = send(turns[n][1], along(1, -1))
        summed.append(gathered(kept[n][0], *came[n], r2r, l2r))
    there = [jnp.concatenate(two, 0) for two in zip(summed[0], summed[1])]
    there = send(second_axis(there), swap_z)
    here = second_axis(summed[2])

    rows_chip = half // 32
    n = rows_chip // 2
    start = ga * half + y * (half // 4) + zl * (half // 8) + x * rows_chip
    row_coul = lax.dynamic_slice_in_dim(coulomb, start, rows_chip, 0)[:, None]
    col_coul = lax.dynamic_slice_in_dim(coulomb, core * 2 * LANES, 2 * LANES, 0)[None, :]
    vmem = pl.BlockSpec(memory_space=pltpu.VMEM)
    shape = jax.ShapeDtypeStruct((2, n, 2 * LANES), jnp.float32)
    keep, give = pl.pallas_call(
        finish_kernel,
        out_shape=[shape, shape],
        in_specs=[pl.BlockSpec(memory_space=pltpu.SMEM)] + [vmem] * 4,
        out_specs=[vmem, vmem],
        name="finish",
    )(jnp.stack([x % 2, core]), here, there, row_coul, col_coul)
    got = send(give, swap_core)
    left = jnp.where(core == 0, keep, got)
    right = jnp.where(core == 0, got, keep)
    return jnp.concatenate([left, right], 2).swapaxes(0, 1)


def solution(mesh):
    finer = Mesh(mesh.devices.reshape(SIZES), AXES)
    band = AXES[:4]
    in_specs = (P(None, band, "ga"), P(band), P(), P(band), P())
    out_specs = P(("ga",) + band, None, None)
    return jax.shard_map(layer, mesh=finer, in_specs=in_specs, out_specs=out_specs, check_vma=False)
```

```python
import functools
import math

import jax
import jax.numpy as jnp
from jax import lax
from jax.experimental import pallas as pl
from jax.experimental.pallas import tpu as pltpu
from jax.sharding import Mesh
from jax.sharding import PartitionSpec as P

LANES = 128
AXES = ("y", "zl", "x", "core", "ga")
SIZES = (4, 2, 4, 2, 2)


def index_of(pos):
    out = 0
    for p, n in zip(pos, SIZES):
        out = out * n + p
    return out


def pairs_of(move):
    pairs = []
    for y in range(4):
        for zl in range(2):
            for x in range(4):
                for core in range(2):
                    for ga in range(2):
                        to = move(y, zl, x, core, ga)
                        if to is not None:
                            pairs.append((index_of((y, zl, x, core, ga)), index_of(to)))
    return pairs


def send(v, move):
    return lax.ppermute(v, AXES, pairs_of(move))


def along(stage, step):
    def move(y, zl, x, core, ga):
        if (core == 0) == (stage == 1):
            return (y, zl, (x + step) % 4, core, ga)
        return ((y + step) % 4, zl, x, core, ga)

    return move


def swap_core(y, zl, x, core, ga):
    return (y, zl, x, 1 - core, ga)


def swap_z(y, zl, x, core, ga):
    return (y, 1 - zl, x, core, ga)


def slab_own(y, zl, x, core, ga):
    return (y, zl, x, core, 1) if ga == 0 else None


def slab_cross(y, zl, x, core, ga):
    return (y, zl, x, 1 - core, 1) if ga == 0 else None


def mm_kernel(
    pos, own, par, coefs, *refs
):
    *slabs, r1, l1, k0, k1, k3, right, col_def, blocks, halves = refs
    chunks = len(slabs) // 4
    out_rows = 2 * chunks * LANES
    core, first, second, ga = pos[1], pos[2], pos[3], pos[4]
    bands, width = own.shape[1:]
    tile = 2 * LANES
    step = pl.program_id(0)

    @pl.when(step == 0)
    def _():
        for chunk in range(chunks):
            own_slab, par_slab, own_far, par_far = slabs[4 * chunk : 4 * chunk + 4]
            total = jnp.zeros((LANES, 1), jnp.float32)
            for which, (near, far) in enumerate(((own_slab, own_far), (par_slab, par_far))):
                coef = coefs[which]
                local = ga == 0
                re = jnp.where(local, near[0], far[0])
                im = jnp.where(local, near[1], far[1])
                defect = coef * (1.0 - 0.5 * (re * re + im * im))
                total = total + jnp.sum(defect.T, axis=1, keepdims=True)
                re_t = (coef * re).T
                im_t = (coef * im).T
                for part, pair in enumerate(((re_t, im_t), (im_t, -re_t))):
                    side = jnp.concatenate(pair, 1)
                    hi = side.astype(jnp.bfloat16)
                    at = pl.ds(which * 2 * bands, 2 * bands)
                    row = (2 * chunk + part) * LANES
                    right[pl.ds(row, LANES), at] = hi
                    right[pl.ds(out_rows + row, LANES), at] = (side - hi.astype(jnp.float32)).astype(
                        jnp.bfloat16
                    )
            col_def[chunk] = jnp.broadcast_to(total, (LANES, LANES))

    dot = functools.partial(jnp.dot, preferred_element_type=jnp.float32)
    lane = lax.broadcasted_iota(jnp.int32, (LANES, LANES), 1)
    low = lane < LANES // 2
    tiles = []
    for start in range(0, width, tile):
        lanes = pl.ds(start, tile)
        rows_def = None
        for which, left in enumerate((own, par)):
            squares = None
            for part in range(2):
                value = left[part, :, lanes]
                squares = value * value if squares is None else squares + value * value
                hi = value.astype(jnp.bfloat16)
                at = pl.ds((2 * which + part) * bands, bands)
                halves[0, at, lanes] = hi
                halves[1, at, lanes] = (value - hi.astype(jnp.float32)).astype(jnp.bfloat16)
            coef = jnp.concatenate([coefs[which]] * 2, 1)
            part_def = jnp.sum(coef * (1.0 - 0.5 * squares), axis=0, keepdims=True)
            rows_def = part_def if rows_def is None else rows_def + part_def
        both = dot(right[...], halves[0, :, lanes])
        acc = both[:out_rows] + both[out_rows:] + dot(right[:out_rows], halves[1, :, lanes])
        for n in range(2):
            cut = slice(n * LANES, (n + 1) * LANES)
            tiles.append((rows_def[:, cut], [acc[m * LANES : (m + 1) * LANES, cut] for m in range(2 * chunks)]))

    for pair in range(width // (3 * LANES)):
        for chunk in range(chunks):
            three = []
            for row_def, parts in tiles[3 * pair : 3 * pair + 3]:
                three.append((parts[2 * chunk] + (row_def + col_def[chunk]), parts[2 * chunk + 1]))
            t0, t1, t2 = three
            turned = (pltpu.roll(t1[0], LANES // 2, 1), pltpu.roll(t1[1], LANES // 2, 1))
            even = (t0[0], t0[1], jnp.where(low, t1[0], turned[1]))
            odd = (t2[0], t2[1], jnp.where(low, turned[0], t1[1]))
            for side, out in enumerate((even, odd)):
                for n, v in enumerate(out):
                    blocks[2 * pair + side, pl.ds((3 * chunk + n) * LANES, LANES), :] = v

    for x in range(4):
        p = jnp.where(core == 0, x, step)
        q = jnp.where(core == 0, step, x)
        rp = lax.rem(p - first + 4, 4)
        rq = lax.rem(q - second + 4, 4)
        half = rq // 2
        place = lax.rem(rq, 2)

        @pl.when(rp == 0)
        def _():
            k0[rq] = blocks[x]

        @pl.when((rp == 1) & (half == 0))
        def _():
            k1[place] = blocks[x]

        @pl.when((rp == 1) & (half == 1))
        def _():
            r1[1, place] = blocks[x]

        @pl.when((rp == 2) & (half == 0))
        def _():
            r1[0, place] = blocks[x]

        @pl.when((rp == 2) & (half == 1))
        def _():
            l1[0, place] = blocks[x]

        @pl.when((rp == 3) & (half == 0))
        def _():
            l1[1, place] = blocks[x]

        @pl.when((rp == 3) & (half == 1))
        def _():
            k3[place] = blocks[x]


def partial_sums(pos, own, par, coefs, far, chunks):
    bands, half = own.shape[1:]
    width = half // 8
    n = len(chunks)
    f32 = jnp.float32
    block = (3 * n * LANES, LANES)
    outs = [(2, 2), (2, 2), (4,), (2,), (2,)]
    left = pl.BlockSpec((2, bands, width), lambda i, pos: (0, 0, 2 * i + pos[0]))

    def whole(*shape):
        return pl.BlockSpec(shape, lambda i, pos: (0,) * len(shape))

    slab = whole(2, bands, LANES)
    in_specs = [left, left, slab]
    operands = [own, par, coefs]
    for chunk in chunks:
        near = pl.BlockSpec(
            (2, bands, LANES), lambda i, pos, chunk=chunk: (0, 0, 2 * pos[1] + chunk)
        )
        in_specs += [near, near, slab, slab]
        operands += [own, par, *far[chunk]]
    return pl.pallas_call(
        mm_kernel,
        out_shape=[jax.ShapeDtypeStruct(o + block, f32) for o in outs],
        grid_spec=pltpu.PrefetchScalarGridSpec(
            num_scalar_prefetch=1,
            grid=(4,),
            in_specs=in_specs,
            out_specs=[whole(*o, *block) for o in outs],
            scratch_shapes=[
                pltpu.VMEM((4 * n * LANES, 4 * bands), jnp.bfloat16),
                pltpu.VMEM((n, LANES, LANES), f32),
                pltpu.VMEM((4,) + block, f32),
                pltpu.VMEM((2, 4 * bands, width), jnp.bfloat16),
            ],
        ),
        compiler_params=pltpu.CompilerParams(
            dimension_semantics=("arbitrary",), vmem_limit_bytes=44 * 2**20
        ),
        cost_estimate=pl.CostEstimate(
            flops=2 * 3 * 2 * n * LANES * 4 * bands * 4 * width,
            bytes_accessed=4 * (16 * bands * width + 16 * block[0] * block[1]),
            transcendentals=0,
        ),
        name="partial_sums",
    )(pos, *operands)


def second_step(k1, k3, r1r, l1r):
    return k1 + r1r[0], k3 + l1r[0]


def gathered(k0, r1r, l1r, r2r, l2r):
    mine = [k0[q] + l1r[1, q] + r2r[q] for q in range(2)]
    return mine + [k0[2 + q] + r1r[1, q] + l2r[q] for q in range(2)]


def second_axis(blocks):
    d1 = send(blocks[1], along(2, 1))
    d3 = send(blocks[3], along(2, -1))
    d2 = send(blocks[2], along(2, 2))
    return blocks[0], d1, d3, d2


def finish_kernel(pos, there, *refs):
    *here, row_coul, col_coul, keep, give = refs
    odd, core = pos[0], pos[1]
    n_rows = row_coul.shape[0] // 2
    for chunk in range(2):
        at = pl.ds(chunk * 3 * LANES, 3 * LANES)
        total = there[at, :]
        if len(here) == 4:
            for ref in here:
                total = total + ref[at, :]
        else:
            for ref in here[:-4] if chunk == 0 else here[-4:]:
                total = total + ref[...]
        body = total[: 2 * LANES].T
        fold = total[2 * LANES :].T
        rest = jnp.concatenate([fold[: LANES // 2], fold[LANES // 2 :]], 1)
        rows = jnp.where(
            odd == 1,
            jnp.concatenate([rest, body], 0),
            jnp.concatenate([body, rest], 0),
        )
        lanes = pl.ds(chunk * LANES, LANES)
        weight = jnp.sqrt(row_coul[...] * col_coul[:, lanes]) * (1.0 / math.sqrt(16384))
        for part in range(2):
            v = weight * rows[:, part * LANES : (part + 1) * LANES]
            top, bottom = v[:n_rows], v[n_rows:]
            keep[part, :, lanes] = jnp.where(core == 0, top, bottom)
            give[part, :, lanes] = jnp.where(core == 0, bottom, top)


def layer(matrix_elements, band_index, occupied, band_weight, coulomb):
    bands, half = matrix_elements.shape[1:]
    y, zl, x, core, ga = (lax.axis_index(a).astype(jnp.int32) for a in AXES)
    occ = (band_index < occupied[0]).astype(jnp.float32)
    coef = (0.5 - occ) * band_weight
    first = jnp.where(core == 0, x, y)
    second = jnp.where(core == 0, y, x)

    own = matrix_elements
    par = send(own, swap_core)
    far = []
    for chunk in range(2):
        pieces = []
        for move, side in ((slab_own, core), (slab_cross, 1 - core)):
            cut = lax.dynamic_slice_in_dim(own, side * 2 * LANES + chunk * LANES, LANES, 2)
            pieces.append(send(cut, move))
        far.append(pieces)
    par_coef = send(coef, swap_core)
    coefs = jnp.broadcast_to(jnp.stack([coef, par_coef])[:, :, None], (2, bands, LANES))

    waves = ((1 - zl, (0,)), (1 - zl, (1,)), (zl, (0,)), (zl, (1,)))
    kept, came = [], []
    for n, (rows_zl, chunks) in enumerate(waves):
        pos = jnp.stack([rows_zl, core, first, second, ga])
        r1, l1, *keep = partial_sums(pos, own, par, coefs, far, chunks)
        kept.append(keep)
        came.append((send(r1, along(1, 1)), send(l1, along(1, -1))))
    summed = []
    for group in ((0,), (1,), (2,), (3,)):
        turn = zip(*(second_step(*kept[n][1:], *came[n]) for n in group))
        r2, l2 = (jnp.concatenate(v, 1) if len(group) > 1 else v[0] for v in turn)
        r2r = send(r2, along(1, 1))
        l2r = send(l2, along(1, -1))
        size = kept[0][0].shape[1]
        for k, n in enumerate(group):
            at = slice(k * size, (k + 1) * size)
            summed.append(gathered(kept[n][0], *came[n], r2r[:, at], l2r[:, at]))
    there = [jnp.concatenate(two, 0) for two in zip(*summed[:2])]
    d0, d1, d3, d2 = second_axis(there)
    there = send(d0 + d1 + d3 + d2, swap_z)
    here = second_axis([jnp.concatenate(two, 0) for two in zip(*summed[2:])])

    rows_chip = half // 32
    n = rows_chip // 2
    start = ga * half + y * (half // 4) + zl * (half // 8) + x * rows_chip
    row_coul = lax.dynamic_slice_in_dim(coulomb, start, rows_chip, 0)[:, None]
    col_coul = lax.dynamic_slice_in_dim(coulomb, core * 2 * LANES, 2 * LANES, 0)[None, :]
    vmem = pl.BlockSpec(memory_space=pltpu.VMEM)
    smem = pl.BlockSpec(memory_space=pltpu.SMEM)
    where = jnp.stack([x % 2, core])
    shape = jax.ShapeDtypeStruct((2, n, 2 * LANES), jnp.float32)
    keep, give = pl.pallas_call(
        finish_kernel,
        out_shape=[shape, shape],
        in_specs=[smem] + [vmem] * (3 + len(here)),
        out_specs=[vmem, vmem],
        name="finish",
    )(where, there, *here, row_coul, col_coul)
    got = send(give, swap_core)
    left = jnp.where(core == 0, keep, got)
    right = jnp.where(core == 0, got, keep)
    return jnp.concatenate([left, right], 2).swapaxes(0, 1)


def solution(mesh):
    finer = Mesh(mesh.devices.reshape(SIZES), AXES)
    band = AXES[:4]
    in_specs = (P(None, band, "ga"), P(band), P(), P(band), P())
    out_specs = P(("ga",) + band, None, None)
    return jax.shard_map(layer, mesh=finer, in_specs=in_specs, out_specs=out_specs, check_vma=False)
```
